32 devices in a mesh: blk: 8 (over y, x, core), grp: 4 (over z).
Axes of the slice: x: 2, y: 2, z: 4, core: 2. Of those that a mesh axis runs over, the one named last changes fastest.
Arguments:
- trial_vec: float32 [1536, 24], P(('blk', 'grp')), may hold values from -6 to 6
- resid_vec: float32 [1536, 24], P(('blk', 'grp')), may hold values from -6 to 6
- search_dir: float32 [1536, 24], P(('blk', 'grp')), may hold values from -6 to 6
- trial_img: float32 [1536, 24], P(('blk', 'grp')), may hold values from -12 to 12
- search_img: float32 [1536, 24], P(('blk', 'grp')), may hold values from -12 to 12
- dens_exch: bfloat16 [1536, 20480], P(('blk', 'grp')), may hold values from -0.15625 to 0.15625
- dens_direct: bfloat16 [1536, 20480], P(('blk', 'grp')), may hold values from -0.15625 to 0.15625
- screen_mat: bfloat16 [20480, 20480], P('grp', 'blk'), may hold values from -0.0390625 to 0.0390625
- coulomb: float32 [20480], replicated, may hold values from 0.2 to 2
- valence_energy: float32 [96], replicated, may hold values from -3 to -1
- conduct_energy: float32 [256], replicated, may hold values from 0.5 to 3
- valence_index: int32 [1536], P(('blk', 'grp')), may hold values from 0 to 95, as said below
- conduct_index: int32 [1536], P(('blk', 'grp')), may hold values from 0 to 255, as said below
- ritz_coef: float32 [72, 24], replicated, may hold values from -1.75 to 1.75
Outputs:
- next_trial: float32 [1536, 24], P(('blk', 'grp'))
- next_trial_img: float32 [1536, 24], P(('blk', 'grp'))
- next_search: float32 [1536, 24], P(('blk', 'grp'))
- next_search_img: float32 [1536, 24], P(('blk', 'grp'))
- gram_matrix: float32 [72, 72], replicated
The draws below stay inside these ranges and needn't reach their ends.
Inputs may be any that keep to these rules, and one draw needn't show every extreme that they name: `valence_index`: no two pairs have both the same valence band and the same conduction band. `conduct_index`: no two pairs have both the same valence band and the same conduction band.
All inputs are finite; a program needn't handle non-finite values.
Results may differ from the reference program's by a relative error of at most 0.0034.
Values may be sent and summed in bfloat16 or wider, within the bound.
A program may use at most 64 MiB of HBM per device.

```python
import math
import jax
import jax.numpy as jnp
from jax import lax

NG = 20480
NE = 24
NV = 96
NC = 256
PAIRS = 1536


def pair_numbers(key):
    mixed = jax.random.permutation(jax.random.fold_in(key, 7), NV * NC)
    return mixed[:PAIRS].astype(jnp.int32)


def draw_valence_index(key, part):
    return (pair_numbers(key) // NC).astype(jnp.int32)


def draw_conduct_index(key, part):
    return (pair_numbers(key) % NC).astype(jnp.int32)


def level_of(own_key, extent, cuts, low, top_value):
    gain = 1.0
    for position, blocks in cuts:
        draws = jax.random.uniform(jax.random.fold_in(jax.random.fold_in(own_key, 6), position), (blocks,), jnp.float32, low / len(cuts), top_value / len(cuts))
        gain = gain * jnp.repeat(jnp.exp(draws), extent[position] // blocks).reshape((-1,) + (1,) * (len(extent) - 1 - position))
    return gain


def bell_draw(key, dims, width, bound, cuts=(), kind=jnp.bfloat16):
    entries = width * jax.random.normal(key, dims, jnp.float32)
    if cuts:
        entries = entries * level_of(key, dims, cuts, -0.22, 0.18)
    return jnp.clip(entries, -bound, bound).astype(kind)


def setup_inputs(seed: int = 0) -> dict:
    keys = jax.random.split(jax.random.key(seed), 15)
    return {
        "trial_vec": bell_draw(keys[0], (PAIRS, NE), 1.0, 6.0, ((0, 32),), jnp.float32),
        "resid_vec": bell_draw(keys[1], (PAIRS, NE), 1.0, 6.0, ((0, 32),), jnp.float32),
        "search_dir": bell_draw(keys[2], (PAIRS, NE), 1.0, 6.0, ((0, 32),), jnp.float32),
        "trial_img": bell_draw(keys[3], (PAIRS, NE), 2.0, 12.0, ((0, 32),), jnp.float32),
        "search_img": bell_draw(keys[4], (PAIRS, NE), 2.0, 12.0, ((0, 32),), jnp.float32),
        "dens_exch": bell_draw(keys[5], (PAIRS, NG), PAIRS ** -0.5, 0.15625, ((0, 32),)),
        "dens_direct": bell_draw(keys[6], (PAIRS, NG), PAIRS ** -0.5, 0.15625, ((0, 32),)),
        "screen_mat": bell_draw(keys[7], (NG, NG), NG ** -0.5, 0.0390625, ((0, 4), (1, 8))),
        "coulomb": jnp.clip(jnp.exp(jax.random.uniform(keys[8], (NG,), jnp.float32, math.log(0.2), math.log(2.0))), 0.2, 2.0),
        "valence_energy": jnp.clip(jax.random.uniform(keys[9], (NV,), jnp.float32, -3.0, -1.0), -3.0, -1.0),
        "conduct_energy": jnp.clip(jax.random.uniform(keys[10], (NC,), jnp.float32, 0.5, 3.0), 0.5, 3.0),
        "valence_index": draw_valence_index(jax.random.fold_in(keys[14], 71), 0),
        "conduct_index": draw_conduct_index(jax.random.fold_in(keys[14], 71), 0),
        "ritz_coef": bell_draw(keys[13], (3 * NE, NE), 0.3, 1.75, (), jnp.float32),
    }


def tdot(left, right):
    return jnp.dot(left, right, precision=lax.Precision.HIGHEST)


def reference(trial_vec, resid_vec, search_dir, trial_img, search_img, dens_exch, dens_direct, screen_mat, coulomb, valence_energy, conduct_energy, valence_index, conduct_index, ritz_coef):
    gap = conduct_energy[conduct_index.astype(jnp.int32)] - valence_energy[valence_index.astype(jnp.int32)]
    resid_half = resid_vec.astype(jnp.bfloat16)
    proj = jnp.dot(dens_exch.T, resid_half, preferred_element_type=jnp.float32)
    weighted = (coulomb[:, None] * proj).astype(jnp.bfloat16)
    exch_term = jnp.dot(dens_exch, weighted, preferred_element_type=jnp.float32)
    seen = jnp.dot(dens_direct.T, resid_half, preferred_element_type=jnp.float32).astype(jnp.bfloat16)
    screened = jnp.dot(screen_mat, seen, preferred_element_type=jnp.float32).astype(jnp.bfloat16)
    direct_term = jnp.dot(dens_direct, screened, preferred_element_type=jnp.float32)
    resid_img = gap[:, None] * resid_vec + 2.0 * exch_term - direct_term
    basis = jnp.concatenate([trial_vec, resid_vec, search_dir], axis=1)
    images = jnp.concatenate([trial_img, resid_img, search_img], axis=1)
    gram_matrix = tdot(basis.T, images)
    lower = ritz_coef[NE:]
    next_trial = tdot(basis, ritz_coef)
    next_trial_img = tdot(images, ritz_coef)
    next_search = tdot(jnp.concatenate([resid_vec, search_dir], axis=1), lower)
    next_search_img = tdot(jnp.concatenate([resid_img, search_img], axis=1), lower)
    return next_trial, next_trial_img, next_search, next_search_img, gram_matrix
```

```python
import functools

import jax
import jax.numpy as jnp
from jax import lax
from jax.experimental import pallas as pl
from jax.experimental.pallas import tpu as pltpu
from jax.sharding import PartitionSpec as P

MESH = pl.DeviceIdType.MESH
F32 = jnp.float32
BF16 = jnp.bfloat16
LANES = 128


def dot_nt(left, right):
    return lax.dot_general(left, right, (((1,), (1,)), ((), ())), preferred_element_type=F32)


def exact(left, right):
    return jnp.dot(left, right, precision=lax.Precision.HIGHEST, preferred_element_type=F32)


def exact_nt(left, right):
    return lax.dot_general(
        left, right, (((1,), (1,)), ((), ())), precision=lax.Precision.HIGHEST,
        preferred_element_type=F32,
    )


def kernel(
    nb, ng, gp, cp,
    trial_vec, resid_vec, search_dir, trial_img, search_img,
    dens_exch, dens_direct, screen_mat, coulomb,
    valence_energy, conduct_energy, valence_index, conduct_index, ritz_coef,
    out_trial, out_trial_img, out_search, out_search_img, out_gram,
    dd, de, ww, pair_out, pair_in, plane_out, plane_in, own_sum, grp_out, grp_in,
    seen_in, seen, fe, fd, part_out, part_in,
    ga_in, ga_mid, gb_in, gb_mid, bas, img, fresh, coef, v_row, c_row,
    load_sem, w_sem, pair_sem, plane_sem, grp_sem, seen_sem, part_sem,
    fe_z, fe_p, fe_c, fd_z, fd_p, fd_c, ga_sem, ga2_sem, gb_sem, gb2_sem,
):
    b = lax.axis_index("blk")
    g = lax.axis_index("grp")
    chips = nb // 2
    c, k = b // 2, b % 2
    total_g = dens_exch.shape[1]
    bc = total_g // nb
    rows = screen_mat.shape[0]
    ne = resid_vec.shape[0]
    ne2 = 2 * ne
    partner = 2 * c + (1 - k)

    def blk_peer(j):
        return lax.rem(b + j, nb)

    def chip_peer(j):
        return lax.rem(c + j, chips)

    def grp_peer(j):
        return lax.rem(g + j, ng)

    def remote(src, dst, sem, idx, dev):
        return pltpu.make_async_remote_copy(
            src_ref=src, dst_ref=dst, send_sem=sem.at[0, idx], recv_sem=sem.at[1, idx],
            device_id=dev, device_id_type=MESH,
        )

    load_d = pltpu.make_async_copy(dens_direct, dd, load_sem.at[0])
    load_e = pltpu.make_async_copy(dens_exch, de, load_sem.at[1])
    load_d.start()
    load_e.start()
    w_loads = []
    for s in range(-(-rows // cp)):
        n = min(cp, rows - s * cp)
        w_loads.append(
            pltpu.make_async_copy(
                screen_mat.at[pl.ds(s * cp, n)], ww.at[s, pl.ds(0, n)], w_sem.at[s]
            )
        )

    barrier = pltpu.get_barrier_semaphore()
    for j in range(1, nb):
        pl.semaphore_signal(barrier, inc=1, device_id=(blk_peer(j), g), device_id_type=MESH)
    for j in range(1, ng):
        pl.semaphore_signal(barrier, inc=1, device_id=(b, grp_peer(j)), device_id_type=MESH)

    pairs = resid_vec.shape[1]
    for ref in (bas, img, fresh, coef, v_row, c_row):
        ref[...] = jnp.zeros_like(ref)
    bas[0:ne, 0:pairs] = trial_vec[...]
    bas[ne:ne2, 0:pairs] = resid_vec[...]
    bas[ne2 : ne2 + ne, 0:pairs] = search_dir[...]
    img[0:ne, 0:pairs] = trial_img[...]
    img[ne2 : ne2 + ne, 0:pairs] = search_img[...]
    coef[:, 0 : ritz_coef.shape[1]] = ritz_coef[...]
    v_row[:, 0 : valence_energy.shape[1]] = valence_energy[...]
    c_row[:, 0 : conduct_energy.shape[1]] = conduct_energy[...]
    resid_t = bas[ne:ne2, 0:pairs]
    half_t = resid_t.astype(BF16)

    def width(q, step, limit):
        return max(0, min(step, limit - q * step))

    def project(blk, q):
        n = width(q, gp, bc)
        off = pl.multiple_of(blk * bc + q * gp, LANES)
        d = jnp.dot(half_t, dd[:, pl.ds(off, n)], preferred_element_type=F32)
        e = jnp.dot(half_t, de[:, pl.ds(off, n)], preferred_element_type=F32)
        return n, jnp.concatenate([d, e], axis=0)

    load_d.wait()
    load_e.wait()
    for copy in w_loads:
        copy.start()
    pl.semaphore_wait(barrier, nb - 1 + ng - 1)

    started = []
    order = list(range(1, chips)) + [0]
    pair = {}
    for j in order:
        dest = chip_peer(j)
        for q in range(ng):
            if width(q, gp, bc):
                n, value = project(2 * dest + (1 - k), q)
                pair_out[j, q, :, pl.ds(0, n)] = value.astype(BF16)
        pair[j] = remote(pair_out.at[j], pair_in.at[j], pair_sem, j, (partner, g))
        pair[j].start()

    plane = {}
    for j in order:
        dest = chip_peer(j)
        pair[j].wait_recv()
        for q in range(ng):
            if width(q, gp, bc):
                n, value = project(2 * dest + k, q)
                value = value + pair_in[j, q, :, pl.ds(0, n)].astype(F32)
                if j:
                    plane_out[j, q, :, pl.ds(0, n)] = value.astype(BF16)
                else:
                    own_sum[q, :, pl.ds(0, n)] = value
        if j:
            plane[j] = remote(
                plane_out.at[j], plane_in.at[j], plane_sem, j, (2 * dest + k, g)
            )
            plane[j].start()

    nv, nc = v_row.shape[1], c_row.shape[1]
    v_hot = lax.broadcasted_iota(jnp.int32, (nv, pairs), 0) == valence_index[...]
    c_hot = lax.broadcasted_iota(jnp.int32, (nc, pairs), 0) == conduct_index[...]
    gap = exact(c_row[...], c_hot.astype(F32)) - exact(v_row[...], v_hot.astype(F32))
    base_t = gap * resid_t
    below = lax.broadcasted_iota(jnp.int32, bas.shape, 0) >= ne
    basis = bas[...]
    old_img = img[...]
    turn = coef[...]
    out_trial[...] = exact(turn, basis)[:, 0:pairs]
    out_search[...] = exact(turn, jnp.where(below, basis, 0.0))[:, 0:pairs]
    img_top = exact(turn, old_img)[:, 0:pairs]
    img_low = exact(turn, jnp.where(below, old_img, 0.0))[:, 0:pairs]
    ga_in[b, 0:ne, :] = exact_nt(old_img[0:ne], basis)
    ga_in[b, ne:ne2, :] = exact_nt(old_img[ne2 : ne2 + ne], basis)
    ga = {}
    for j in range(1, nb):
        ga[j] = remote(ga_in.at[b], ga_in.at[b], ga_sem, j, (blk_peer(j), g))

    for j in range(1, chips):
        plane[j].wait_recv()

    zsum = {}
    own_q = None
    def plane_total(q):
        value = own_sum[q]
        for j in range(1, chips):
            value = value + plane_in[j, q].astype(F32)
        return value

    for j in range(1, ng):
        q = grp_peer(j)
        grp_out[j] = plane_total(q).astype(BF16)
        zsum[j] = remote(grp_out.at[j], grp_in.at[j], grp_sem, j, (b, q))
        zsum[j].start()
    value = plane_total(g)
    for j in range(1, ng):
        zsum[j].wait_recv()
        value = value + grp_in[j].astype(F32)
    seen_in[g] = value[0:ne].astype(BF16)
    sz = {}
    for j in range(1, ng):
        sz[j] = remote(seen_in.at[g], seen_in.at[g], seen_sem, j, (b, grp_peer(j)))
        sz[j].start()
    c_off = b * bc + g * gp
    if ng * gp != bc:
        c_off = jnp.minimum(c_off, total_g - gp)
    fe[b, g] = (coulomb[:, pl.ds(pl.multiple_of(c_off, LANES), gp)] * value[ne:]).astype(BF16)

    def gather_grp(buf, sem):
        out = {}
        for j in range(1, ng):
            out[j] = remote(buf.at[b, g], buf.at[b, g], sem, j, (b, grp_peer(j)))
            out[j].start()
        return out

    def gather_chips(buf, sem, core_sem):
        out = {}
        for j in range(1, chips):
            out[j] = remote(buf.at[b], buf.at[b], sem, j, (2 * chip_peer(j) + k, g))
            out[j].start()
        core = {0: remote(buf.at[b], buf.at[b], core_sem, 0, (partner, g))}
        core[0].start()
        return out, core

    def from_chip(j):
        return 2 * lax.rem(c + chips - j, chips) + k

    def pass_on(buf, arrived, core, core_sem):
        for j in range(1, chips):
            arrived[j].wait_recv()
            src = from_chip(j)
            core[j] = remote(buf.at[src], buf.at[src], core_sem, j, (partner, g))
            core[j].start()

    ez = gather_grp(fe, fe_z)
    for copy in w_loads:
        copy.wait()
    for j in range(1, ng):
        sz[j].wait_recv()
    for q in range(ng):
        n = width(q, gp, bc)
        if n:
            seen[:, pl.ds(q * gp, n)] = seen_in[q, :, pl.ds(0, n)]

    seen_value = seen[...]
    parts = {}
    ep = ec = None
    for j in list(range(1, nb)) + [0]:
        dest = blk_peer(j)
        value = dot_nt(seen_value, ww[dest])
        if j:
            part_out[j] = value.astype(BF16)
            parts[j] = remote(part_out.at[j], part_in.at[j], part_sem, j, (dest, g))
            parts[j].start()
        if j == 1:
            for i in range(1, ng):
                ez[i].wait_recv()
            ep, ec = gather_chips(fe, fe_p, fe_c)
            for i in range(1, nb):
                ga[i].start()

    for j in range(1, nb):
        parts[j].wait_recv()
        value = value + part_in[j].astype(F32)
    fd[b, g] = value.astype(BF16)
    dz = gather_grp(fd, fd_z)

    def wait_all(copies):
        for copy in copies.values():
            copy.wait_recv()

    pass_on(fe, ep, ec, fe_c)
    wait_all(ga)
    for r in range(nb):
        ga_sum = ga_in[r] if r == 0 else ga_sum + ga_in[r]
    ga_mid[g] = ga_sum
    ga2 = {}
    for j in range(1, ng):
        ga2[j] = remote(ga_mid.at[g], ga_mid.at[g], ga2_sem, j, (b, grp_peer(j)))
        ga2[j].start()

    def exch_block(src, acc):
        for q in range(ng):
            n = width(q, gp, bc)
            if n:
                off = pl.multiple_of(src * bc + q * gp, LANES)
                acc = acc + dot_nt(fe[src, q, :, pl.ds(0, n)], de[:, pl.ds(off, n)])
        return acc

    def direct_block(src, acc):
        for q in range(ng):
            off = src * cp + q * rows
            if nb * cp != rows:
                off = jnp.minimum(off, total_g - cp)
            term = dot_nt(fd[src, q], dd[:, pl.ds(pl.multiple_of(off, LANES), cp)])
            if nb * cp != rows:
                term = jnp.where(src * cp < rows, term, 0.0)
            acc = acc + term
        return acc

    wait_all(dz)
    dp, dc = gather_chips(fd, fd_p, fd_c)

    acc = jnp.zeros((ne, pairs), F32)
    for j in range(chips):
        acc = exch_block(from_chip(j), acc)
    wait_all(ec)
    for j in range(chips):
        acc = exch_block(from_chip(j) + 1 - 2 * k, acc)
    acc_d = direct_block(b, jnp.zeros((ne, pairs), F32))
    dc[0].wait_recv()
    acc_d = direct_block(partner, acc_d)
    pass_on(fd, dp, dc, fd_c)
    for j in range(1, chips):
        acc_d = direct_block(from_chip(j), acc_d)
    for j in range(1, chips):
        dc[j].wait_recv()
        acc_d = direct_block(from_chip(j) + 1 - 2 * k, acc_d)

    img_t = base_t + 2.0 * acc - acc_d
    fresh[ne:ne2, 0:pairs] = img_t
    gb_in[b] = exact_nt(fresh[ne:ne2], basis)
    gb = {}
    for j in range(1, nb):
        gb[j] = remote(gb_in.at[b], gb_in.at[b], gb_sem, j, (blk_peer(j), g))
        gb[j].start()
    turned = exact(turn, fresh[...])[:, 0:pairs]
    out_search_img[...] = turned + img_low
    out_trial_img[...] = turned + img_top
    wait_all(ga2)
    for r in range(ng):
        ga_tot = ga_mid[r] if r == 0 else ga_tot + ga_mid[r]
    wait_all(gb)
    for r in range(nb):
        gb_sum = gb_in[r] if r == 0 else gb_sum + gb_in[r]
    gb_mid[g] = gb_sum
    gb2 = {}
    for j in range(1, ng):
        gb2[j] = remote(gb_mid.at[g], gb_mid.at[g], gb2_sem, j, (b, grp_peer(j)))
        gb2[j].start()
    wait_all(gb2)
    for r in range(ng):
        gb_tot = gb_mid[r] if r == 0 else gb_tot + gb_mid[r]
    gram_t = jnp.concatenate([ga_tot[0:ne], gb_tot, ga_tot[ne:]], axis=0)
    out_gram[...] = gram_t.T[0 : 3 * ne, :]

    for group in (pair, plane, zsum, sz, ez, ep, ec, parts, dz, dp, dc, ga, ga2, gb, gb2):
        for copy in group.values():
            copy.wait_send()


def up(size):
    return -(-size // LANES) * LANES


def shards(
    trial_vec, resid_vec, search_dir, trial_img, search_img, dens_exch, dens_direct,
    screen_mat, coulomb, valence_energy, conduct_energy, valence_index, conduct_index, ritz_coef,
):
    nb, ng = lax.axis_size("blk"), lax.axis_size("grp")
    pairs, ne = resid_vec.shape
    rows, bc = screen_mat.shape
    gp = -(-bc // (ng * LANES)) * LANES
    cp = -(-rows // (nb * LANES)) * LANES
    chips = nb // 2
    ne2 = 2 * ne
    total_g = dens_exch.shape[1]
    vmem = pl.BlockSpec(memory_space=pltpu.VMEM)
    hbm = pl.BlockSpec(memory_space=pl.ANY)
    sems = lambda n: pltpu.SemaphoreType.DMA((2, n))
    small = jax.ShapeDtypeStruct((ne, pairs), F32)
    side, wide = up(3 * ne), up(pairs)
    outs = pl.pallas_call(
        functools.partial(kernel, nb, ng, gp, cp),
        out_shape=(small, small, small, small, jax.ShapeDtypeStruct((3 * ne, 3 * ne), F32)),
        in_specs=[vmem] * 5 + [hbm] * 3 + [vmem] * 6,
        out_specs=(vmem,) * 5,
        scratch_shapes=[
            pltpu.VMEM((pairs, total_g), BF16),
            pltpu.VMEM((pairs, total_g), BF16),
            pltpu.VMEM((nb, cp, bc), BF16),
            pltpu.VMEM((chips, ng, ne2, gp), BF16),
            pltpu.VMEM((chips, ng, ne2, gp), BF16),
            pltpu.VMEM((chips, ng, ne2, gp), BF16),
            pltpu.VMEM((chips, ng, ne2, gp), BF16),
            pltpu.VMEM((ng, ne2, gp), F32),
            pltpu.VMEM((ng, ne2, gp), BF16),
            pltpu.VMEM((ng, ne2, gp), BF16),
            pltpu.VMEM((ng, ne, gp), BF16),
            pltpu.VMEM((ne, bc), BF16),
            pltpu.VMEM((nb, ng, ne, gp), BF16),
            pltpu.VMEM((nb, ng, ne, cp), BF16),
            pltpu.VMEM((nb, ne, cp), BF16),
            pltpu.VMEM((nb, ne, cp), BF16),
            pltpu.VMEM((nb, ne2, side), F32),
            pltpu.VMEM((ng, ne2, side), F32),
            pltpu.VMEM((nb, ne, side), F32),
            pltpu.VMEM((ng, ne, side), F32),
            pltpu.VMEM((side, wide), F32),
            pltpu.VMEM((side, wide), F32),
            pltpu.VMEM((side, wide), F32),
            pltpu.VMEM((ne, side), F32),
            pltpu.VMEM((1, up(valence_energy.shape[0])), F32),
            pltpu.VMEM((1, up(conduct_energy.shape[0])), F32),
            pltpu.SemaphoreType.DMA((2,)),
            pltpu.SemaphoreType.DMA((nb,)),
            sems(chips), sems(chips), sems(ng), sems(ng), sems(nb),
            sems(ng), sems(chips), sems(chips), sems(ng), sems(chips), sems(chips),
            sems(nb), sems(ng), sems(nb), sems(ng),
        ],
        compiler_params=pltpu.CompilerParams(
            collective_id=0, has_side_effects=True, vmem_limit_bytes=60 * 1024 * 1024
        ),
    )(
        trial_vec.T, resid_vec.T, search_dir.T, trial_img.T, search_img.T, dens_exch, dens_direct,
        screen_mat, coulomb[None, :], valence_energy[None, :], conduct_energy[None, :],
        valence_index[None, :], conduct_index[None, :], ritz_coef.T,
    )
    return tuple(x.T for x in outs[:4]) + (outs[4],)


def solution(mesh):
    rows = P(("blk", "grp"), None)
    return jax.shard_map(
        shards,
        mesh=mesh,
        in_specs=(rows,) * 7
        + (P("grp", "blk"), P(), P(), P(), P(("blk", "grp")), P(("blk", "grp")), P()),
        out_specs=(rows,) * 4 + (P(),),
        check_vma=False,
    )
```

```python
import functools

import jax
import jax.numpy as jnp
from jax import lax
from jax.experimental import pallas as pl
from jax.experimental.pallas import tpu as pltpu
from jax.sharding import PartitionSpec as P

MESH = pl.DeviceIdType.MESH
F32 = jnp.float32
BF16 = jnp.bfloat16
LANES = 128


def dot_nt(left, right):
    return lax.dot_general(left, right, (((1,), (1,)), ((), ())), preferred_element_type=F32)


def exact(left, right):
    return jnp.dot(left, right, precision=lax.Precision.HIGHEST, preferred_element_type=F32)


def exact_nt(left, right):
    return lax.dot_general(
        left, right, (((1,), (1,)), ((), ())), precision=lax.Precision.HIGHEST,
        preferred_element_type=F32,
    )


def kernel(
    nb, ng, gp, cp,
    trial_vec, resid_vec, search_dir, trial_img, search_img,
    dens_exch, dens_direct, screen_mat, coulomb,
    valence_energy, conduct_energy, valence_index, conduct_index, ritz_coef,
    packed,
    dd, de, ww, pair_out, pair_in, plane_out, plane_in, own_sum, grp_out, grp_in,
    seen_in, seen, fe, fd, part_out, part_in,
    ga_in, ga_mid, gb_in, gb_mid, bas, img, fresh, coef, v_row, c_row,
    load_sem, w_sem, pair_sem, plane_sem, grp_sem, seen_sem, part_sem,
    fe_z, fe_p, fe_c, fd_z, fd_p, fd_c, ga_sem, ga2_sem, gb_sem, gb2_sem,
):
    b = lax.axis_index("blk")
    g = lax.axis_index("grp")
    chips = nb // 2
    c, k = b // 2, b % 2
    total_g = dens_exch.shape[1]
    bc = total_g // nb
    rows = screen_mat.shape[0]
    ne = resid_vec.shape[0]
    ne2 = 2 * ne
    partner = 2 * c + (1 - k)

    def blk_peer(j):
        return lax.rem(b + j, nb)

    def chip_peer(j):
        return lax.rem(c + j, chips)

    def grp_peer(j):
        return lax.rem(g + j, ng)

    def remote(src, dst, sem, idx, dev):
        return pltpu.make_async_remote_copy(
            src_ref=src, dst_ref=dst, send_sem=sem.at[0, idx], recv_sem=sem.at[1, idx],
            device_id=dev, device_id_type=MESH,
        )

    load_d = pltpu.make_async_copy(dens_direct, dd, load_sem.at[0])
    load_e = pltpu.make_async_copy(dens_exch, de, load_sem.at[1])
    load_d.start()
    load_e.start()
    w_loads = []
    for s in range(-(-rows // cp)):
        n = min(cp, rows - s * cp)
        w_loads.append(
            pltpu.make_async_copy(
                screen_mat.at[pl.ds(s * cp, n)], ww.at[s, pl.ds(0, n)], w_sem.at[s]
            )
        )

    barrier = pltpu.get_barrier_semaphore()
    for j in range(1, nb):
        pl.semaphore_signal(barrier, inc=1, device_id=(blk_peer(j), g), device_id_type=MESH)
    for j in range(1, ng):
        pl.semaphore_signal(barrier, inc=1, device_id=(b, grp_peer(j)), device_id_type=MESH)

    pairs = resid_vec.shape[1]
    for ref in (bas, img, fresh, coef, v_row, c_row):
        ref[...] = jnp.zeros_like(ref)
    bas[0:ne, 0:pairs] = trial_vec[...]
    bas[ne:ne2, 0:pairs] = resid_vec[...]
    bas[ne2 : ne2 + ne, 0:pairs] = search_dir[...]
    img[0:ne, 0:pairs] = trial_img[...]
    img[ne2 : ne2 + ne, 0:pairs] = search_img[...]
    coef[:, 0 : ritz_coef.shape[1]] = ritz_coef[...]
    v_row[:, 0 : valence_energy.shape[1]] = valence_energy[...]
    c_row[:, 0 : conduct_energy.shape[1]] = conduct_energy[...]
    resid_t = bas[ne:ne2, 0:pairs]
    half_t = resid_t.astype(BF16)

    def width(q, step, limit):
        return max(0, min(step, limit - q * step))

    def project(blk, q):
        n = width(q, gp, bc)
        off = pl.multiple_of(blk * bc + q * gp, LANES)
        d = jnp.dot(half_t, dd[:, pl.ds(off, n)], preferred_element_type=F32)
        e = jnp.dot(half_t, de[:, pl.ds(off, n)], preferred_element_type=F32)
        return n, jnp.concatenate([d, e], axis=0)

    load_d.wait()
    load_e.wait()
    for copy in w_loads:
        copy.start()
    pl.semaphore_wait(barrier, nb - 1 + ng - 1)

    started = []
    order = list(range(1, chips)) + [0]
    pair = {}
    for j in order:
        dest = chip_peer(j)
        for q in range(ng):
            if width(q, gp, bc):
                n, value = project(2 * dest + (1 - k), q)
                pair_out[j, q, :, pl.ds(0, n)] = value.astype(BF16)
        pair[j] = remote(pair_out.at[j], pair_in.at[j], pair_sem, j, (partner, g))
        pair[j].start()

    plane = {}
    for j in order:
        dest = chip_peer(j)
        pair[j].wait_recv()
        for q in range(ng):
            if width(q, gp, bc):
                n, value = project(2 * dest + k, q)
                value = value + pair_in[j, q, :, pl.ds(0, n)].astype(F32)
                if j:
                    plane_out[j, q, :, pl.ds(0, n)] = value.astype(BF16)
                else:
                    own_sum[q, :, pl.ds(0, n)] = value
        if j:
            plane[j] = remote(
                plane_out.at[j], plane_in.at[j], plane_sem, j, (2 * dest + k, g)
            )
            plane[j].start()

    nv, nc = v_row.shape[1], c_row.shape[1]
    v_hot = lax.broadcasted_iota(jnp.int32, (nv, pairs), 0) == valence_index[...]
    c_hot = lax.broadcasted_iota(jnp.int32, (nc, pairs), 0) == conduct_index[...]
    gap = exact(c_row[...], c_hot.astype(F32)) - exact(v_row[...], v_hot.astype(F32))
    base_t = gap * resid_t
    below = lax.broadcasted_iota(jnp.int32, bas.shape, 0) >= ne
    basis = bas[...]
    old_img = img[...]
    turn = coef[...]
    packed[0 * ne : 1 * ne, 0:pairs] = exact(turn, basis)[:, 0:pairs]
    packed[2 * ne : 3 * ne, 0:pairs] = exact(turn, jnp.where(below, basis, 0.0))[:, 0:pairs]
    img_top = exact(turn, old_img)[:, 0:pairs]
    img_low = exact(turn, jnp.where(below, old_img, 0.0))[:, 0:pairs]
    ga_in[b, 0:ne, :] = exact_nt(old_img[0:ne], basis)
    ga_in[b, ne:ne2, :] = exact_nt(old_img[ne2 : ne2 + ne], basis)
    ga = {}
    for j in range(1, nb):
        ga[j] = remote(ga_in.at[b], ga_in.at[b], ga_sem, j, (blk_peer(j), g))

    for j in range(1, chips):
        plane[j].wait_recv()

    zsum = {}
    own_q = None
    def plane_total(q):
        value = own_sum[q]
        for j in range(1, chips):
            value = value + plane_in[j, q].astype(F32)
        return value

    for j in range(1, ng):
        q = grp_peer(j)
        grp_out[j] = plane_total(q).astype(BF16)
        zsum[j] = remote(grp_out.at[j], grp_in.at[j], grp_sem, j, (b, q))
        zsum[j].start()
    value = plane_total(g)
    for j in range(1, ng):
        zsum[j].wait_recv()
        value = value + grp_in[j].astype(F32)
    seen_in[g] = value[0:ne].astype(BF16)
    sz = {}
    for j in range(1, ng):
        sz[j] = remote(seen_in.at[g], seen_in.at[g], seen_sem, j, (b, grp_peer(j)))
        sz[j].start()
    c_off = b * bc + g * gp
    if ng * gp != bc:
        c_off = jnp.minimum(c_off, total_g - gp)
    fe[b, g] = (coulomb[:, pl.ds(pl.multiple_of(c_off, LANES), gp)] * value[ne:]).astype(BF16)

    def gather_grp(buf, sem):
        out = {}
        for j in range(1, ng):
            out[j] = remote(buf.at[b, g], buf.at[b, g], sem, j, (b, grp_peer(j)))
            out[j].start()
        return out

    def gather_chips(buf, sem, core_sem):
        out = {}
        for j in range(1, chips):
            out[j] = remote(buf.at[b], buf.at[b], sem, j, (2 * chip_peer(j) + k, g))
            out[j].start()
        core = {0: remote(buf.at[b], buf.at[b], core_sem, 0, (partner, g))}
        core[0].start()
        return out, core

    def from_chip(j):
        return 2 * lax.rem(c + chips - j, chips) + k

    def pass_on(buf, arrived, core, core_sem):
        for j in range(1, chips):
            arrived[j].wait_recv()
            src = from_chip(j)
            core[j] = remote(buf.at[src], buf.at[src], core_sem, j, (partner, g))
            core[j].start()

    ez = gather_grp(fe, fe_z)
    for copy in w_loads:
        copy.wait()
    for j in range(1, ng):
        sz[j].wait_recv()
    for q in range(ng):
        n = width(q, gp, bc)
        if n:
            seen[:, pl.ds(q * gp, n)] = seen_in[q, :, pl.ds(0, n)]

    seen_value = seen[...]
    parts = {}
    ep = ec = None
    for j in list(range(1, nb)) + [0]:
        dest = blk_peer(j)
        value = dot_nt(ww[dest], seen_value).T
        if j:
            part_out[j] = value.astype(BF16)
            parts[j] = remote(part_out.at[j], part_in.at[j], part_sem, j, (dest, g))
            parts[j].start()
        if j == 1:
            for i in range(1, ng):
                ez[i].wait_recv()
            ep, ec = gather_chips(fe, fe_p, fe_c)
            for i in range(1, nb):
                ga[i].start()

    for j in range(1, nb):
        parts[j].wait_recv()
        value = value + part_in[j].astype(F32)
    fd[b, g] = value.astype(BF16)
    dz = gather_grp(fd, fd_z)
    dp, dc = {}, {}

    def spread(z):
        q = lax.rem(g + ng - z, ng)
        for i in range(1, chips):
            dp[i, z] = remote(
                fd.at[b, q], fd.at[b, q], fd_p, i * ng + z, (2 * chip_peer(i) + k, g)
            )
            dp[i, z].start()
        dc[0, z] = remote(fd.at[b, q], fd.at[b, q], fd_c, z, (partner, g))
        dc[0, z].start()

    spread(0)

    def wait_all(copies):
        for copy in copies.values():
            copy.wait_recv()

    pass_on(fe, ep, ec, fe_c)
    wait_all(ga)
    for r in range(nb):
        ga_sum = ga_in[r] if r == 0 else ga_sum + ga_in[r]
    ga_mid[g] = ga_sum
    ga2 = {}
    for j in range(1, ng):
        ga2[j] = remote(ga_mid.at[g], ga_mid.at[g], ga2_sem, j, (b, grp_peer(j)))
        ga2[j].start()

    def exch_block(src, acc):
        for q in range(ng):
            n = width(q, gp, bc)
            if n:
                off = pl.multiple_of(src * bc + q * gp, LANES)
                acc = acc + dot_nt(fe[src, q, :, pl.ds(0, n)], de[:, pl.ds(off, n)])
        return acc

    def direct_piece(src, z, acc):
        q = lax.rem(g + ng - z, ng)
        off = src * cp + q * rows
        if nb * cp != rows:
            off = jnp.minimum(off, total_g - cp)
        term = dot_nt(fd[src, q], dd[:, pl.ds(pl.multiple_of(off, LANES), cp)])
        if nb * cp != rows:
            term = jnp.where(src * cp < rows, term, 0.0)
        return acc + term

    for z in range(1, ng):
        dz[z].wait_recv()
        spread(z)

    acc = jnp.zeros((ne, pairs), F32)
    for j in range(chips):
        acc = exch_block(from_chip(j), acc)
    wait_all(ec)
    for j in range(chips):
        acc = exch_block(from_chip(j) + 1 - 2 * k, acc)
    acc_d = jnp.zeros((ne, pairs), F32)
    for z in range(ng):
        for i in range(1, chips):
            dp[i, z].wait_recv()
            src = from_chip(i)
            q = lax.rem(g + ng - z, ng)
            dc[i, z] = remote(fd.at[src, q], fd.at[src, q], fd_c, i * ng + z, (partner, g))
            dc[i, z].start()
        for i in range(chips):
            acc_d = direct_piece(from_chip(i), z, acc_d)
    for z in range(ng):
        for i in range(chips):
            dc[i, z].wait_recv()
        for i in range(chips):
            acc_d = direct_piece(from_chip(i) + 1 - 2 * k, z, acc_d)

    img_t = base_t + 2.0 * acc - acc_d
    fresh[ne:ne2, 0:pairs] = img_t
    gb_in[b] = exact_nt(fresh[ne:ne2], basis)
    gb = {}
    for j in range(1, nb):
        gb[j] = remote(gb_in.at[b], gb_in.at[b], gb_sem, j, (blk_peer(j), g))
        gb[j].start()
    turned = exact(turn, fresh[...])[:, 0:pairs]
    packed[3 * ne : 4 * ne, 0:pairs] = turned + img_low
    packed[1 * ne : 2 * ne, 0:pairs] = turned + img_top
    wait_all(ga2)
    for r in range(ng):
        ga_tot = ga_mid[r] if r == 0 else ga_tot + ga_mid[r]
    wait_all(gb)
    for r in range(nb):
        gb_sum = gb_in[r] if r == 0 else gb_sum + gb_in[r]
    gb_mid[g] = gb_sum
    gb2 = {}
    for j in range(1, ng):
        gb2[j] = remote(gb_mid.at[g], gb_mid.at[g], gb2_sem, j, (b, grp_peer(j)))
        gb2[j].start()
    wait_all(gb2)
    for r in range(ng):
        gb_tot = gb_mid[r] if r == 0 else gb_tot + gb_mid[r]
    gram_t = jnp.concatenate([ga_tot[0:ne], gb_tot, ga_tot[ne:]], axis=0)
    packed[4 * ne : 7 * ne, 0 : 3 * ne] = gram_t.T[0 : 3 * ne, :]

    for group in (pair, plane, zsum, sz, ez, ep, ec, parts, dz, dp, dc, ga, ga2, gb, gb2):
        for copy in group.values():
            copy.wait_send()


def unpack(packed, *outs):
    row = 0
    for out in outs:
        n, m = out.shape
        out[...] = packed[row : row + n, 0:m]
        row += n


def up(size):
    return -(-size // LANES) * LANES


def shards(
    trial_vec, resid_vec, search_dir, trial_img, search_img, dens_exch, dens_direct,
    screen_mat, coulomb, valence_energy, conduct_energy, valence_index, conduct_index, ritz_coef,
):
    nb, ng = lax.axis_size("blk"), lax.axis_size("grp")
    pairs, ne = resid_vec.shape
    rows, bc = screen_mat.shape
    gp = -(-bc // (ng * LANES)) * LANES
    cp = -(-rows // (nb * LANES)) * LANES
    chips = nb // 2
    ne2 = 2 * ne
    total_g = dens_exch.shape[1]
    vmem = pl.BlockSpec(memory_space=pltpu.VMEM)
    hbm = pl.BlockSpec(memory_space=pl.ANY)
    sems = lambda n: pltpu.SemaphoreType.DMA((2, n))
    small = jax.ShapeDtypeStruct((ne, pairs), F32)
    side, wide = up(3 * ne), up(pairs)
    joined = pl.pallas_call(
        functools.partial(kernel, nb, ng, gp, cp),
        out_shape=jax.ShapeDtypeStruct((7 * ne, max(side, wide)), F32),
        in_specs=[vmem] * 5 + [hbm] * 3 + [vmem] * 6,
        out_specs=vmem,
        scratch_shapes=[
            pltpu.VMEM((pairs, total_g), BF16),
            pltpu.VMEM((pairs, total_g), BF16),
            pltpu.VMEM((nb, cp, bc), BF16),
            pltpu.VMEM((chips, ng, ne2, gp), BF16),
            pltpu.VMEM((chips, ng, ne2, gp), BF16),
            pltpu.VMEM((chips, ng, ne2, gp), BF16),
            pltpu.VMEM((chips, ng, ne2, gp), BF16),
            pltpu.VMEM((ng, ne2, gp), F32),
            pltpu.VMEM((ng, ne2, gp), BF16),
            pltpu.VMEM((ng, ne2, gp), BF16),
            pltpu.VMEM((ng, ne, gp), BF16),
            pltpu.VMEM((ne, bc), BF16),
            pltpu.VMEM((nb, ng, ne, gp), BF16),
            pltpu.VMEM((nb, ng, ne, cp), BF16),
            pltpu.VMEM((nb, ne, cp), BF16),
            pltpu.VMEM((nb, ne, cp), BF16),
            pltpu.VMEM((nb, ne2, side), F32),
            pltpu.VMEM((ng, ne2, side), F32),
            pltpu.VMEM((nb, ne, side), F32),
            pltpu.VMEM((ng, ne, side), F32),
            pltpu.VMEM((side, wide), F32),
            pltpu.VMEM((side, wide), F32),
            pltpu.VMEM((side, wide), F32),
            pltpu.VMEM((ne, side), F32),
            pltpu.VMEM((1, up(valence_energy.shape[0])), F32),
            pltpu.VMEM((1, up(conduct_energy.shape[0])), F32),
            pltpu.SemaphoreType.DMA((2,)),
            pltpu.SemaphoreType.DMA((nb,)),
            sems(chips), sems(chips), sems(ng), sems(ng), sems(nb),
            sems(ng), sems(chips), sems(chips), sems(ng), sems(chips * ng), sems(chips * ng),
            sems(nb), sems(ng), sems(nb), sems(ng),
        ],
        compiler_params=pltpu.CompilerParams(
            collective_id=0, has_side_effects=True, vmem_limit_bytes=60 * 1024 * 1024
        ),
    )(
        trial_vec.T, resid_vec.T, search_dir.T, trial_img.T, search_img.T, dens_exch, dens_direct,
        screen_mat, coulomb[None, :], valence_energy[None, :], conduct_energy[None, :],
        valence_index[None, :], conduct_index[None, :], ritz_coef.T,
    )
    outs = pl.pallas_call(
        unpack,
        out_shape=(small,) * 4 + (jax.ShapeDtypeStruct((3 * ne, 3 * ne), F32),),
        in_specs=[vmem],
        out_specs=(vmem,) * 5,
    )(joined)
    return tuple(x.T for x in outs[:4]) + (outs[4],)


def solution(mesh):
    rows = P(("blk", "grp"), None)
    return jax.shard_map(
        shards,
        mesh=mesh,
        in_specs=(rows,) * 7
        + (P("grp", "blk"), P(), P(), P(), P(("blk", "grp")), P(("blk", "grp")), P()),
        out_specs=(rows,) * 4 + (P(),),
        check_vma=False,
    )
```
